32 devices in a mesh: row: 4 (over z), col: 4 (over x, core), layer: 2 (over y).
Axes of the slice: x: 2, y: 2, z: 4, core: 2. Of those that a mesh axis runs over, the one named last changes fastest.
Arguments:
- left: bfloat16 [4096, 8192], P('row', ('col', 'layer')), may hold values from -6 to 6
- middle: bfloat16 [8192, 8192], P('row', 'col'), may hold values from -0.0625 to 0.0625
- right: bfloat16 [8192, 8192], P('row', 'col'), may hold values from -0.0625 to 0.0625
Outputs:
- product: bfloat16 [4096, 8192], P('row', ('col', 'layer'))
The draws below stay inside these ranges and needn't reach their ends.
All inputs are finite; a program needn't handle non-finite values.
Results may differ from the reference program's by a relative error of at most 0.0049.
Values may be sent and summed in bfloat16 or wider, within the bound.
A program may use at most 128 MiB of HBM per device.

```python
import jax
import jax.numpy as jnp

K = 8192
N = 8192
P_SIZE = 8192
M = 4096


def block_scale(rng, dims, pieces, low, high):
    loudness, own = 1.0, jax.random.fold_in(rng, 6)
    for axis_at, shards_of in pieces:
        heights = jnp.exp(jax.random.uniform(jax.random.fold_in(own, axis_at), (shards_of,), jnp.float32, low / len(pieces), high / len(pieces)))
        loudness = loudness * jnp.repeat(heights, dims[axis_at] // shards_of).reshape([-1 if axis == axis_at else 1 for axis in range(len(dims))])
    return loudness


def scatter_about(key, dims, deviation, limit, shards=(), kind=jnp.bfloat16):
    array = jax.random.normal(key, dims, jnp.float32) * deviation
    if len(shards) > 0:
        array = block_scale(key, dims, shards, -0.22, 0.18) * array
    return jnp.clip(array, min=-limit, max=limit).astype(kind)


def setup_inputs(seed: int = 0) -> dict:
    streams_of = jax.random.split(jax.random.key(seed), 4)
    return {
        "left": scatter_about(streams_of[0], (M, K), 1.0, 6.0, ((0, 4), (1, 8))),
        "middle": scatter_about(streams_of[1], (K, N), K ** -0.5, 0.0625, ((0, 4), (1, 4))),
        "right": scatter_about(streams_of[2], (N, P_SIZE), N ** -0.5, 0.0625, ((0, 4), (1, 4))),
    }


def reference(left, middle, right):
    first = jnp.dot(left, middle, preferred_element_type=jnp.float32).astype(jnp.bfloat16)
    return jnp.dot(first, right, preferred_element_type=jnp.float32).astype(jnp.bfloat16)
```

```python
import functools

import jax
import jax.numpy as jnp
from jax import lax
from jax.experimental import pallas as pl
from jax.experimental.pallas import tpu as pltpu
from jax.sharding import PartitionSpec as P

CHUNKS = 4
TILE = 256
PAIR = 2
PIECES = 8
INNER = (
    (0,), (1,), (2, 1), (2, 0), (4, 0, 0), (4, 0, 1), (4, 0, 2), (4, 0, 3), (6, 0, 0), (4, 0, 4), (4, 0, 5),
    (4, 0, 6), (5, 0), (9, 0), (6, 0, 1), (10, 1), (16, 0, 1), (4, 0, 7), (3, 0), (6, 0, 2), (6, 0, 3), (10, 0),
    (3, 1), (5, 1), (6, 0, 4), (16, 0, 0), (6, 0, 5), (10, 2), (16, 0, 2), (10, 3), (16, 0, 3), (4, 1, 0),
    (8, 0, 1, 0), (9, 1), (6, 0, 6), (4, 1, 1), (7, 0, 0), (16, 1, 1), (16, 1, 2), (4, 1, 2), (7, 0, 1), (10, 4),
    (16, 0, 4), (4, 1, 3), (16, 1, 3), (7, 0, 2), (16, 1, 4), (4, 1, 4), (16, 1, 0), (15, 1, 0), (7, 0, 3), (4, 1, 5),
    (7, 1, 0), (6, 0, 7), (4, 1, 6), (15, 1, 1), (7, 1, 1), (4, 1, 7), (15, 1, 2), (10, 5), (16, 0, 5), (16, 1, 5),
    (15, 0, 1), (7, 1, 2), (15, 0, 0), (7, 1, 3), (7, 0, 4), (15, 0, 2), (7, 1, 4), (15, 1, 3), (10, 6), (16, 0, 6),
    (16, 1, 6), (15, 0, 3), (10, 7), (8, 1, 1, 0), (8, 1, 1, 1), (7, 0, 5), (15, 1, 4), (7, 1, 5), (16, 0, 7),
    (15, 0, 4), (16, 1, 7), (8, 1, 0, 0), (15, 1, 5), (8, 1, 1, 2), (8, 1, 0, 1), (15, 0, 5), (7, 0, 6), (7, 1, 6),
    (15, 1, 6), (8, 1, 1, 3), (8, 1, 0, 3), (5, 2), (15, 0, 6), (8, 1, 1, 6), (8, 1, 0, 2), (7, 0, 7), (7, 1, 7),
    (15, 1, 7), (8, 1, 1, 4), (6, 1, 0), (15, 0, 7), (8, 1, 0, 4), (8, 1, 1, 5), (8, 1, 0, 5), (8, 0, 2, 0), (9, 2),
    (16, 2, 0), (15, 2, 0), (8, 1, 1, 7), (11, 0), (6, 1, 1), (16, 2, 4), (11, 4), (8, 1, 0, 6), (14, 1), (16, 2, 1),
    (11, 1), (16, 2, 2), (11, 2), (8, 1, 0, 7), (16, 2, 3), (11, 3), (12, 0), (16, 2, 6), (7, 2, 0), (16, 2, 5),
    (15, 2, 1), (14, 0), (11, 5), (13, 0), (16, 2, 7), (11, 6), (15, 2, 2), (8, 1, 2, 0), (11, 7), (6, 1, 2),
    (17, 1, 0), (15, 2, 3), (7, 2, 1), (7, 2, 2), (12, 1), (7, 2, 3), (15, 2, 4), (6, 1, 3), (13, 1), (17, 1, 1),
    (15, 2, 5), (15, 2, 6), (7, 2, 4), (7, 2, 5), (12, 2), (7, 2, 6), (13, 2), (17, 1, 2), (18, 0), (7, 2, 7),
    (8, 1, 2, 1), (15, 2, 7), (6, 1, 4), (8, 1, 2, 2), (18, 1), (12, 3), (13, 3), (17, 1, 3), (8, 1, 2, 3),
    (8, 1, 2, 4), (8, 1, 2, 5), (6, 1, 5), (8, 1, 2, 6), (8, 1, 2, 7), (14, 2), (17, 2, 0), (17, 2, 1), (17, 2, 2),
    (6, 1, 6), (17, 2, 3), (18, 2), (6, 1, 7), (12, 4), (13, 4), (17, 2, 4), (17, 1, 4), (18, 3), (12, 5), (13, 5),
    (17, 2, 5), (17, 1, 5), (12, 6), (13, 6), (17, 2, 6), (17, 1, 6), (18, 4), (12, 7), (13, 7), (17, 2, 7),
    (17, 1, 7), (18, 5), (18, 6), (18, 7),
)
OUTER = (
    (4, 0, 0), (0,), (4, 0, 1), (4, 0, 2), (4, 0, 3), (6, 0, 0), (10, 0), (6, 0, 1), (6, 0, 2), (4, 0, 4), (4, 0, 5),
    (4, 0, 6), (10, 1), (4, 0, 7), (6, 0, 3), (5, 0), (2, 0), (1,), (2, 1), (3, 0), (3, 1), (9, 0), (16, 0, 0),
    (11, 0), (16, 0, 1), (11, 1), (7, 0, 0), (10, 2), (7, 0, 1), (16, 0, 2), (6, 0, 4), (11, 2), (10, 3), (7, 0, 2),
    (16, 0, 3), (6, 0, 5), (10, 4), (7, 0, 3), (16, 0, 4), (6, 0, 6), (11, 3), (7, 0, 6), (11, 4), (10, 5), (7, 0, 4),
    (16, 0, 5), (7, 0, 5), (6, 0, 7), (11, 5), (10, 6), (16, 0, 6), (6, 1, 0), (11, 6), (10, 7), (4, 1, 0),
    (16, 0, 7), (6, 1, 1), (7, 0, 7), (4, 1, 1), (4, 1, 2), (6, 1, 2), (4, 1, 3), (12, 0), (4, 1, 4), (13, 0),
    (4, 1, 5), (6, 1, 3), (12, 1), (4, 1, 6), (6, 1, 4), (13, 1), (4, 1, 7), (12, 2), (6, 1, 5), (12, 3), (6, 1, 6),
    (13, 2), (12, 4), (6, 1, 7), (13, 3), (12, 5), (12, 6), (11, 7), (13, 4), (15, 0, 0), (8, 1, 0, 0), (12, 7),
    (13, 5), (15, 0, 1), (13, 6), (15, 0, 2), (8, 1, 0, 1), (15, 0, 3), (13, 7), (8, 1, 0, 3), (15, 0, 4), (15, 0, 5),
    (8, 1, 0, 2), (8, 1, 0, 4), (15, 0, 6), (8, 1, 0, 5), (8, 1, 0, 6), (15, 0, 7), (8, 1, 0, 7), (14, 0), (18, 0),
    (18, 1), (18, 2), (18, 3), (18, 4), (18, 5), (18, 6), (18, 7),
)
MESH = pl.DeviceIdType.MESH


def kernel(
    rows, cols, layers,
    left_ref, middle_ref, right_ref, out_ref,
    held, held2, rhs, sent, kept, near, far, near2,
    own_sem, home_sem, swap_sems, pair_sems, plane_sems, core_sems, near_sems, far_sems, near2_sems, hop_sems, relay_sems,
):
    group, side = rows // 2, cols // 2
    row, col, layer = lax.axis_index("row"), lax.axis_index("col"), lax.axis_index("layer")
    h, z = row // group, lax.rem(row, group)
    x, c = col // side, lax.rem(col, side)
    straight = h == x
    depth = middle_ref.shape[0]
    width = out_ref.shape[1]
    inner = left_ref.shape[1]
    chunk = left_ref.shape[0] // CHUNKS
    tile = min(TILE, width)

    def at(h_, x_):
        return (h_ * group + z, x_ * side + c, layer)

    def slot(col_, layer_):
        return col_ * layers + layer_

    sibling = col + 1 - 2 * lax.rem(col, 2)
    offsets = [(dc, dl) for dc in range(cols // 2) for dl in range(layers) if dc or dl]

    def moved(col_, dc, dl, sign):
        return lax.rem(col_ + sign * 2 * dc + cols, cols), lax.rem(layer + sign * dl + layers, layers)

    barrier = pltpu.get_barrier_semaphore()
    greeted = [at(1 - h, x), at(h, 1 - x), at(1 - h, 1 - x), (row, sibling, layer)]
    for shift in range(1, group):
        greeted.append((h * group + lax.rem(z + shift, group), col, layer))
    for dc, dl in offsets:
        greeted.append((row, *moved(col, dc, dl, 1)))
    for device in greeted:
        pl.semaphore_signal(barrier, inc=1, device_id=device, device_id_type=MESH)
    pl.semaphore_wait(barrier, len(greeted))

    me = slot(col, layer)

    def part(j):
        return pl.ds(j * chunk, chunk)

    def remote(src, dst, sems, device):
        return pltpu.make_async_remote_copy(
            src_ref=src, dst_ref=dst, send_sem=sems.at[0], recv_sem=sems.at[1],
            device_id=device, device_id_type=MESH,
        )

    home = pltpu.make_async_copy(left_ref, held.at[me], home_sem)

    def swap(j):
        device = at(1 - h, x) if j % 2 else at(h, 1 - x)
        return remote(left_ref.at[part(j)], near2.at[part(j)], swap_sems.at[j], device)

    def hop(j):
        device = at(h, 1 - x) if j % 2 else at(1 - h, x)
        target = slot((1 - x) * side + c, layer) if j % 2 else me
        return remote(near2.at[part(j)], held.at[target, part(j)], hop_sems.at[j], device)

    columns = pl.ds(pl.multiple_of(layer * width, width), width)
    pieces = CHUNKS
    step = depth // pieces

    def own(which):
        ref = (middle_ref, right_ref)[which]
        return pltpu.make_async_copy(
            ref.at[:, columns], rhs.at[which, pl.ds(z * depth, depth)], own_sem.at[which]
        )

    def pair(which, piece, shift):
        ref = (middle_ref, right_ref)[which]
        return remote(
            ref.at[pl.ds(piece * step, step), columns],
            rhs.at[which, pl.ds(z * depth + piece * step, step)],
            pair_sems.at[which, piece, shift - 1],
            (h * group + lax.rem(z + shift, group), col, layer),
        )

    def pair_start(which, piece):
        for shift in range(1, group):
            pair(which, piece, shift).start()

    def pair_wait(which):
        for piece in range(pieces):
            for shift in range(1, group):
                pair(which, piece, shift).wait_recv()
        own(which).wait()

    buffers = (held, held2)

    def spread(phase, j, index):
        dc, dl = offsets[index]
        ref = buffers[phase].at[me, part(j)]
        return remote(ref, ref, plane_sems.at[phase, j, index], (row, *moved(col, dc, dl, 1)))

    def pass_on(phase, j, index):
        origin = me
        if index:
            dc, dl = offsets[index - 1]
            origin = slot(*moved(col, dc, dl, -1))
        ref = buffers[phase].at[origin, part(j)]
        return remote(ref, ref, core_sems.at[phase, j, index], (row, sibling, layer))

    def spread_start(phase, j):
        for index in range(len(offsets)):
            spread(phase, j, index).start()
        pass_on(phase, j, 0).start()

    def spread_finish(phase, j):
        for index in range(len(offsets)):
            spread(phase, j, index).wait_recv()
            pass_on(phase, j, index + 1).start()
        for index in range(len(offsets) + 1):
            pass_on(phase, j, index).wait_recv()

    def multiply(phase, j, piece, target):
        blocks = side * layers
        ref = buffers[phase]

        @pl.loop(0, width // tile)
        def _(n):
            across = pl.ds(pl.multiple_of(n * tile, tile), tile)
            total = jnp.zeros((chunk, tile), jnp.float32)
            for k in range(blocks):
                total += jnp.dot(
                    ref[piece * blocks + k, part(j), :],
                    rhs[phase, pl.ds(k * inner, inner), across],
                    preferred_element_type=jnp.float32,
                )
            target[part(j), across] = total.astype(target.dtype)

    def add(one, two, j, store):
        @pl.loop(0, chunk // 32)
        def _(i):
            span = pl.ds(pl.multiple_of(j * chunk + i * 32, 32), 32)
            value = one[span, :].astype(jnp.float32) + two[span, :].astype(jnp.float32)
            store(span, value.astype(jnp.bfloat16))

    def near_copy(j):
        target_row = jnp.where(straight, h, x)
        target_col = jnp.where(straight, 1 - x, x)
        return remote(sent.at[part(j)], near.at[part(j)], near_sems.at[j], at(target_row, target_col))

    def far_copy(j):
        return remote(kept.at[part(j)], far.at[part(j)], far_sems.at[j], at(h, 1 - x))

    def relay_copy(j):
        return remote(far.at[part(j)], far.at[part(j)], relay_sems.at[j], at(1 - h, x))

    def near2_copy(j):
        return remote(sent.at[part(j)], near2.at[part(j)], near2_sems.at[j], at(1 - h, x))

    @pl.when(straight)
    def _():
        home.start()

    @pl.when(jnp.logical_not(straight))
    def _():
        for j in range(CHUNKS):
            swap(j).start()

    own(0).start()
    own(1).start()
    for piece in range(pieces):
        pair_start(0, piece)

    @pl.when(straight)
    def _():
        home.wait()

    for j in range(CHUNKS):
        @pl.when(straight)
        def _():
            swap(j).wait_recv()
            hop(j).start()

        @pl.when(jnp.logical_not(straight))
        def _():
            hop(j).wait_recv()

        spread_start(0, j)

    @pl.when(straight)
    def _():
        for j in range(CHUNKS):
            hop(j).wait_send()

    def first_done(j):
        near_copy(j).wait_recv()

        def store(span, value):
            held2[me, span, :] = value

        @pl.when(straight)
        def _():
            add(near, kept, j, store)

        @pl.when(jnp.logical_not(straight))
        def _():
            relay_copy(j).wait_recv()
            add(near, far, j, store)

        spread_start(1, j)

    for j in range(CHUNKS):
        spread_finish(0, j)
        if j == 0:
            pair_wait(0)
        multiply(0, j, h, kept)

        @pl.when(jnp.logical_not(straight))
        def _():
            far_copy(j).start()

        multiply(0, j, 1 - h, sent)
        near_copy(j).start()

        @pl.when(straight)
        def _():
            far_copy(j).wait_recv()
            relay_copy(j).start()

        pair_start(1, j)
        if j:
            first_done(j - 1)
    first_done(CHUNKS - 1)

    def out_done(j):
        near2_copy(j).wait_recv()

        def store(span, value):
            out_ref[span, :] = value

        add(near2, kept, j, store)

    for j in range(CHUNKS):
        spread_finish(1, j)
        if j == 0:
            pair_wait(1)
        near_copy(j).wait_send()

        @pl.when(jnp.logical_not(straight))
        def _():
            far_copy(j).wait_send()

        multiply(1, j, 1 - h, sent)
        near2_copy(j).start()
        multiply(1, j, h, kept)
        if j:
            out_done(j - 1)
    out_done(CHUNKS - 1)

    @pl.when(jnp.logical_not(straight))
    def _():
        for j in range(CHUNKS):
            swap(j).wait_send()

    @pl.when(straight)
    def _():
        for j in range(CHUNKS):
            relay_copy(j).wait_send()

    for j in range(CHUNKS):
        near2_copy(j).wait_send()
        for phase in range(2):
            for index in range(len(offsets)):
                spread(phase, j, index).wait_send()
            for index in range(len(offsets) + 1):
                pass_on(phase, j, index).wait_send()
    for which in range(2):
        for piece in range(pieces):
            for shift in range(1, group):
                pair(which, piece, shift).wait_send()


def wide_kernel(
    rows, cols, layers,
    left_ref, middle_ref, right_ref, out_ref, stage,
    a, b, part, cross, remote, pre, turned, far, fin,
    a_local, turn_sem, a_send, a_recv, pre_sems, own_sems, load_sems, bz_sems, by_sems,
    sx_sems, sc_sems, cross_sems, fwd_send, fwd_recv, o_send, o_recv, f_sems,
):
    group, side = rows // 2, cols // 2
    z, col, y = lax.axis_index("row"), lax.axis_index("col"), lax.axis_index("layer")
    x, c = col // side, lax.rem(col, side)
    h, par = z // group, lax.rem(z, group)
    straight = x == h
    crossed = jnp.logical_not(straight)
    inner = par != h
    mate = h * group + 1 - par
    near_z = (1 - h) * group + h
    far_z = (1 - h) * group + 1 - h
    depth = middle_ref.shape[0]
    width = middle_ref.shape[1]
    deep = left_ref.shape[1]
    half = left_ref.shape[0] // layers
    quarter = half // 2
    w = width // PIECES
    slabs = 3

    def at(z_, x_, c_, y_):
        return (z_, x_ * side + c_, y_)

    greeted = []
    for dx in range(2):
        for dc in range(2):
            for dy in range(2):
                if dx or dc or dy:
                    greeted.append(at(z, lax.rem(x + dx, 2), lax.rem(c + dc, 2), lax.rem(y + dy, 2)))
    for dz in range(1, rows):
        for dy in range(2):
            greeted.append(at(lax.rem(z + dz, rows), x, c, lax.rem(y + dy, 2)))
    barrier = pltpu.get_barrier_semaphore()
    for device in greeted:
        pl.semaphore_signal(barrier, inc=1, device_id=device, device_id_type=MESH)

    def send(src, dst, send_sem, recv_sem, device):
        return pltpu.make_async_remote_copy(
            src_ref=src, dst_ref=dst, send_sem=send_sem, recv_sem=recv_sem,
            device_id=device, device_id_type=MESH,
        )

    def when(flag, call, *args):
        @pl.when(flag)
        def _():
            call(*args)

    def left_rows(y_, s):
        return left_ref.at[pl.ds(pl.multiple_of(y_ * half + s * quarter, quarter), quarter)]

    def left_half(y_):
        return left_ref.at[pl.ds(pl.multiple_of(y_ * half, half), half)]

    def deep_cols(y_):
        return pl.ds(pl.multiple_of(y_ * deep, deep), deep)

    def rows_of(s):
        return pl.ds(pl.multiple_of(s * quarter, quarter), quarter)

    def a_piece(slab, s, y_):
        return a.at[0, slab, c, rows_of(s), deep_cols(y_)]

    def a_half(y_):
        return a.at[0, 0, c, :, deep_cols(y_)]

    there = jnp.where(inner, 1, 2)

    def keep_left():
        return pltpu.make_async_copy(left_half(y), a_half(y), a_local)

    def turn_kept():
        return send(left_half(1 - y), a_half(y), a_send.at[0], a_recv.at[0, y], at(z, x, c, 1 - y))

    def turn_sent():
        return send(left_half(1 - y), turned, a_send.at[0], turn_sem, at(z, x, c, 1 - y))

    def side_left(k):
        y_ = 1 - y if k else y
        return send(a_half(y_) if k else left_half(y), a_half(y_), a_send.at[1 + k], a_recv.at[0, y_], at(z, 1 - x, c, y))

    def give_left(k):
        src = turned.at[rows_of(1 - x)] if k else left_rows(y, 1 - x)
        return send(src, pre.at[k], a_send.at[1 + k], pre_sems.at[k], at(z, 1 - x, c, y))

    def jump(src, k):
        y_ = 1 - y if k else y
        return send(src, a_piece(there, x, y_), a_send.at[3 + k], a_recv.at[there, y_], at(near_z, x, c, y))

    def jump_left(k):
        return jump(turned.at[rows_of(x)] if k else left_rows(y, x), k)

    def left_start():
        @pl.when(straight)
        def _():
            turn_kept().start()
            side_left(0).start()
            keep_left().start()

        @pl.when(crossed)
        def _():
            turn_sent().start()
            give_left(0).start()

    def left_give():
        @pl.when(crossed)
        def _():
            turn_sent().wait_recv()
            give_left(1).start()

    def left_jump(k):
        @pl.when(crossed)
        def _():
            jump_left(k).start()

    def left_relay(k):
        @pl.when(straight)
        def _():
            give_left(k).wait_recv()
            jump(pre.at[k], k).start()

    def a_in(slab):
        def arrived(y_):
            ref = a_piece(slab, x, y_) if slab else a_half(y_)
            send(ref, ref, a_send.at[0], a_recv.at[slab, y_], at(z, x, c, 1 - y)).wait_recv()

        if slab:
            arrived(0)
            arrived(1)
            spread_x(0, slab, 0, x).start()
            spread_c(0, slab, 0, 0).start()
        else:
            @pl.when(straight)
            def _():
                arrived(1 - y)
                side_left(1).start()
                keep_left().wait()

            @pl.when(crossed)
            def _():
                arrived(0)
                arrived(1)

            whole(0).start()

    def a_block(phase, slab, s, n):
        if phase:
            return a.at[1, slab, c, rows_of(s), strip(n)]
        return a.at[0, slab, c, rows_of(s)]

    def spread_x(phase, slab, n, s):
        ref = a_block(phase, slab, s, n)
        k = n + phase
        return send(ref, ref, sx_sems.at[slab, k, 0], sx_sems.at[slab, k, 1], at(z, 1 - x, c, y))

    def spread_c(phase, slab, n, which):
        ref = a_block(phase, slab, 1 - x if which else x, n)
        k = n + phase
        return send(ref, ref, sc_sems.at[slab, k, which, 0], sc_sems.at[slab, k, which, 1], at(z, x, 1 - c, y))

    def whole(_):
        ref = a.at[0, 0, c]
        return send(ref, ref, sc_sems.at[0, 0, 0, 0], sc_sems.at[0, 0, 0, 1], at(z, x, 1 - c, y))

    def pass_on(phase, slab, n):
        spread_x(phase, slab, n, 1 - x).wait_recv()
        spread_c(phase, slab, n, 1).start()

    def a_ready(slab):
        if slab:
            for which in range(2):
                spread_c(0, slab, 0, which).wait_recv()
        else:
            whole(0).wait_recv()

    def a2_ready(slab):
        for n in range(PIECES):
            for which in range(2):
                spread_c(1, slab, n, which).wait_recv()

    sources = (middle_ref, right_ref)

    def strip(n):
        return pl.ds(n * w, w)

    def b_rows(plane, y_):
        return pl.ds(pl.multiple_of(plane * depth + y_ * (depth // 2), depth // 2), depth // 2)

    def b_slot(phase, n, plane, y_):
        if phase:
            return stage.at[n, b_rows(0, y_)]
        return b.at[n, b_rows(plane, y_)]

    def bz(phase, n):
        src = sources[phase].at[b_rows(0, y), strip(n)]
        return send(src, b_slot(phase, n, par, y), bz_sems.at[phase, n, 0], bz_sems.at[phase, n, 1], at(mate, x, c, y))

    def by(phase, n):
        ref = b_slot(phase, n, 1 - par, y)
        return send(ref, ref, by_sems.at[phase, n, 0], by_sems.at[phase, n, 1], at(z, x, c, 1 - y))

    def own(phase, n):
        rows_ = pl.ds(pl.multiple_of(par * depth, depth), depth)
        return pltpu.make_async_copy(sources[phase].at[:, strip(n)], b.at[n, rows_], own_sems.at[phase, n])

    def load(n):
        rows_ = pl.ds(pl.multiple_of((1 - par) * depth, depth), depth)
        return pltpu.make_async_copy(stage.at[n], b.at[n, rows_], load_sems.at[n])

    def b_send(phase, n):
        bz(phase, n).start()

    def b_turn(phase, n):
        bz(phase, n).wait_recv()
        by(phase, n).start()

    def b_ready(n):
        own(0, n).wait()
        by(0, n).wait_recv()

    def b_own(n):
        own(1, n).start()

    def b_load(n):
        by(0, n).wait_send()
        by(1, n).wait_recv()
        load(n).start()

    def b_loaded(n):
        own(1, n).wait()
        load(n).wait()

    def multiply(phase, slab, n, store):
        def add(k, total):
            deep_rows = pl.ds(pl.multiple_of(k * deep, deep), deep)
            cols_ = pl.ds(pl.multiple_of(lax.rem(k, 2) * deep, deep), deep)
            return total + jnp.dot(a[phase, slab, k // 2, :, cols_], b[n, deep_rows], preferred_element_type=jnp.float32)

        store(n, lax.fori_loop(0, 2 * depth // deep, add, jnp.zeros((half, w), jnp.float32)))

    def keep(slab):
        def store(n, total):
            part[slab, :, strip(n)] = total.astype(part.dtype)

        return store

    home_slab = (jnp.where(inner, 1, 2), 0, 0)
    home_z = (near_z, near_z, far_z)

    def cross_copy(slab, n):
        return send(
            part.at[slab, rows_of(1 - x), strip(n)], cross.at[slab, :, strip(n)],
            cross_sems.at[slab, n, 0], cross_sems.at[slab, n, 1], at(z, 1 - x, c, y),
        )

    def fwd_copy(slab, n, src):
        to = home_slab[slab]
        return send(
            src, remote.at[to, :, strip(n)], fwd_send.at[slab, n], fwd_recv.at[to, n],
            at(home_z[slab], x, c, y),
        )

    def fwd_part(slab, n):
        return fwd_copy(slab, n, part.at[slab, rows_of(x), strip(n)])

    def fwd_cross(slab, n):
        return fwd_copy(slab, n, cross.at[slab, :, strip(n)])

    def unit1(slab, n):
        multiply(0, slab, n, keep(slab))
        cross_copy(slab, n).start()

        @pl.when(crossed)
        def _():
            fwd_part(slab, n).start()

    def relay1(slab, n):
        @pl.when(straight)
        def _():
            cross_copy(slab, n).wait_recv()
            fwd_cross(slab, n).start()

    def reduce1(slab, n):
        ref = remote.at[slab, :, strip(n)]
        send(ref, ref, fwd_send.at[slab, n], fwd_recv.at[slab, n], at(z, x, c, 1 - y)).wait_recv()

        def add(other, base):
                @pl.loop(0, quarter // 32)
                def _(i):
                    span = pl.ds(pl.multiple_of(i * 32, 32), 32)
                    into = pl.ds(pl.multiple_of(x * quarter + i * 32, 32), 32)
                    mine = pl.ds(pl.multiple_of(base + i * 32, 32), 32)
                    value = other[slab, mine, strip(n)].astype(jnp.float32) + remote[slab, span, strip(n)].astype(jnp.float32)
                    a[1, slab, c, into, strip(n)] = value.astype(a.dtype)

        @pl.when(straight)
        def _():
            add(part, x * quarter)

        @pl.when(crossed)
        def _():
            cross_copy(slab, n).wait_recv()
            add(cross, 0)

        spread_x(1, slab, n, x).start()
        spread_c(1, slab, n, 0).start()

    def out_copy(slab, n):
        return send(
            part.at[slab, :, strip(n)], far.at[:, strip(n)], o_send.at[slab - 1, n], o_recv.at[n],
            at(home_z[slab], x, c, y),
        )

    def unit2(slab, n):
        cross_copy(slab, n).wait_send()
        fwd_part(slab, n).wait_send()
        multiply(1, slab, n, keep(slab))
        out_copy(slab, n).start()

    my_rows = pl.ds(pl.multiple_of(y * half, half), half)

    def fin_copy(n):
        cols_ = pl.ds(n % (PIECES // 2) * w, w)
        return send(fin.at[n], out_ref.at[my_rows, cols_], f_sems.at[n, 0], f_sems.at[n, 1], at(z, x, c, 1 - y))

    def unit3(n):
        ref = far.at[:, strip(n)]
        send(ref, ref, o_send.at[0, n], o_recv.at[n], at(z, x, c, 1 - y)).wait_recv()

        def store(n, total):
            value = total + far[:, strip(n)].astype(jnp.float32)
            fin[n] = value.astype(fin.dtype)

        multiply(1, 0, n, store)
        mine = y == n // (PIECES // 2)

        @pl.when(mine)
        def _():
            out_ref[my_rows, pl.ds(n % (PIECES // 2) * w, w)] = fin[n]

        @pl.when(jnp.logical_not(mine))
        def _():
            fin_copy(n).start()

    steps = (
        left_start, left_give, left_jump, left_relay, b_send, a_in, b_turn, relay1, pass_on, a_ready,
        b_ready, b_own, b_load, b_loaded, a2_ready, reduce1, unit1, unit2, unit3,
    )
    for n in range(PIECES):
        own(0, n).start()
    pl.semaphore_wait(barrier, len(greeted))

    def follow(order):
        for step, *args in order:
            steps[step](*args)

    when(inner, follow, INNER)
    when(jnp.logical_not(inner), follow, OUTER)

    for n in range(PIECES):
        mine = y == n // (PIECES // 2)

        @pl.when(mine)
        def _():
            fin_copy(n).wait_recv()

        @pl.when(jnp.logical_not(mine))
        def _():
            fin_copy(n).wait_send()

    @pl.when(straight)
    def _():
        turn_kept().wait_send()
        for k in range(2):
            side_left(k).wait_send()
            jump(pre.at[k], k).wait_send()

    @pl.when(crossed)
    def _():
        turn_sent().wait_send()
        for k in range(2):
            give_left(k).wait_send()
            jump_left(k).wait_send()

    for phase in range(2):
        for n in range(PIECES):
            bz(phase, n).wait_send()
            if phase:
                by(phase, n).wait_send()

    def sent(slab):
        if slab:
            spread_x(0, slab, 0, x).wait_send()
            for which in range(2):
                spread_c(0, slab, 0, which).wait_send()
        else:
            whole(0).wait_send()
        for n in range(PIECES):
            spread_x(1, slab, n, x).wait_send()
            for which in range(2):
                spread_c(1, slab, n, which).wait_send()
            if slab:
                out_copy(slab, n).wait_send()
            else:
                cross_copy(slab, n).wait_send()
                fwd_part(slab, n).wait_send()

    sent(0)
    for slab in range(1, slabs):
        when(inner, sent, slab)


def wide(rows, cols, layers, left, middle, right):
    height, inner = left.shape
    depth, width = middle.shape
    half = height // layers
    quarter = half // 2
    bf16 = jnp.bfloat16
    anywhere = pl.BlockSpec(memory_space=pl.ANY)
    dma = pltpu.SemaphoreType.DMA
    out, _ = pl.pallas_call(
        functools.partial(wide_kernel, rows, cols, layers),
        out_shape=(
            jax.ShapeDtypeStruct((height, width // layers), bf16),
            jax.ShapeDtypeStruct((PIECES, depth, width // PIECES), bf16),
        ),
        in_specs=[anywhere] * 3,
        out_specs=(pl.BlockSpec(memory_space=pltpu.VMEM), anywhere),
        scratch_shapes=[
            pltpu.VMEM((2, 3, 2, half, depth), bf16),
            pltpu.VMEM((PIECES, 2 * depth, width // PIECES), bf16),
            pltpu.VMEM((3, half, width), bf16),
            pltpu.VMEM((3, quarter, width), bf16),
            pltpu.VMEM((3, quarter, width), bf16),
            pltpu.VMEM((2, quarter, inner), bf16),
            pltpu.VMEM((half, inner), bf16),
            pltpu.VMEM((half, width), bf16),
            pltpu.VMEM((PIECES, half, width // PIECES), bf16),
            dma,
            dma,
            dma((5,)),
            dma((3, 2)),
            dma((2,)),
            dma((2, PIECES)),
            dma((PIECES,)),
            dma((2, PIECES, 2)),
            dma((2, PIECES, 2)),
            dma((3, PIECES + 1, 2)),
            dma((3, PIECES + 1, 2, 2)),
            dma((3, PIECES, 2)),
            dma((3, PIECES)),
            dma((3, PIECES)),
            dma((2, PIECES)),
            dma((PIECES,)),
            dma((PIECES, 2)),
        ],
        compiler_params=pltpu.CompilerParams(
            collective_id=0, has_side_effects=True, vmem_limit_bytes=67043328
        ),
    )(left, middle, right)
    return out


def per_device(left, middle, right):
    rows, cols, layers = (lax.axis_size(name) for name in ("row", "col", "layer"))
    height, inner = left.shape
    width = right.shape[1] // layers
    depth = right.shape[0]
    group = rows // 2
    if (rows, cols, layers) == (2 * PAIR, 2 * PAIR, PAIR) and depth == layers * inner:
        return wide(rows, cols, layers, left, middle, right)
    partners = cols // 2 * layers - 1
    bf16 = jnp.bfloat16
    anywhere = pl.BlockSpec(memory_space=pl.ANY)
    dma = pltpu.SemaphoreType.DMA
    return pl.pallas_call(
        functools.partial(kernel, rows, cols, layers),
        out_shape=jax.ShapeDtypeStruct((height, width), bf16),
        in_specs=[anywhere] * 3,
        out_specs=pl.BlockSpec(memory_space=pltpu.VMEM),
        scratch_shapes=[
            pltpu.VMEM((cols * layers, height, inner), bf16),
            pltpu.VMEM((cols * layers, height, inner), bf16),
            pltpu.VMEM((2, group * depth, width), bf16),
        ]
        + [pltpu.VMEM((height, width), bf16)] * 5
        + [
            dma((2,)),
            dma,
            dma((CHUNKS, 2)),
            dma((2, CHUNKS, max(group - 1, 1), 2)),
            dma((2, CHUNKS, partners, 2)),
            dma((2, CHUNKS, partners + 1, 2)),
            dma((CHUNKS, 2)),
            dma((CHUNKS, 2)),
            dma((CHUNKS, 2)),
            dma((CHUNKS, 2)),
            dma((CHUNKS, 2)),
        ],
        compiler_params=pltpu.CompilerParams(
            collective_id=0, has_side_effects=True, vmem_limit_bytes=67043328
        ),
    )(left, middle, right)


def solution(mesh):
    return jax.shard_map(
        per_device,
        mesh=mesh,
        in_specs=(P("row", ("col", "layer")), P("row", "col"), P("row", "col")),
        out_specs=P("row", ("col", "layer")),
        check_vma=False,
    )
```

```python
import functools

import jax
import jax.numpy as jnp
from jax import lax
from jax.experimental import pallas as pl
from jax.experimental.pallas import tpu as pltpu
from jax.sharding import PartitionSpec as P

CHUNKS = 4
TILE = 256
PAIR = 2
PIECES = 8
INNER = (
    (0,), (1,), (2, 1), (2, 0), (4, 0, 0), (4, 0, 1), (4, 0, 2), (4, 0, 3), (6, 0, 0), (4, 0, 4), (4, 0, 5),
    (4, 0, 6), (5, 0), (9, 0), (6, 0, 1), (10, 1), (16, 0, 1), (4, 0, 7), (3, 0), (6, 0, 2), (6, 0, 3), (10, 0),
    (3, 1), (5, 1), (6, 0, 4), (16, 0, 0), (6, 0, 5), (10, 2), (16, 0, 2), (10, 3), (16, 0, 3), (4, 1, 0),
    (8, 0, 1, 0), (9, 1), (6, 0, 6), (4, 1, 1), (7, 0, 0), (16, 1, 1), (16, 1, 2), (4, 1, 2), (7, 0, 1), (10, 4),
    (16, 0, 4), (4, 1, 3), (16, 1, 3), (7, 0, 2), (16, 1, 4), (4, 1, 4), (16, 1, 0), (15, 1, 0), (7, 0, 3), (4, 1, 5),
    (7, 1, 0), (6, 0, 7), (4, 1, 6), (15, 1, 1), (7, 1, 1), (4, 1, 7), (15, 1, 3), (15, 1, 2), (10, 5), (16, 0, 5),
    (16, 1, 5), (15, 0, 1), (7, 1, 2), (15, 0, 0), (7, 1, 3), (7, 0, 4), (15, 0, 2), (7, 1, 4), (10, 6), (16, 0, 6),
    (16, 1, 6), (15, 0, 3), (10, 7), (8, 1, 1, 0), (8, 1, 1, 1), (7, 0, 5), (15, 1, 4), (7, 1, 5), (16, 0, 7),
    (15, 0, 4), (16, 1, 7), (8, 1, 0, 0), (15, 1, 5), (8, 1, 1, 2), (8, 1, 0, 1), (15, 0, 5), (7, 0, 6), (7, 1, 6),
    (15, 1, 6), (8, 1, 1, 3), (8, 1, 0, 3), (5, 2), (15, 0, 6), (8, 1, 1, 6), (8, 1, 0, 2), (7, 0, 7), (7, 1, 7),
    (15, 1, 7), (8, 1, 1, 4), (6, 1, 0), (15, 0, 7), (8, 1, 0, 4), (8, 1, 1, 5), (8, 1, 0, 5), (8, 0, 2, 0), (9, 2),
    (16, 2, 0), (15, 2, 0), (8, 1, 1, 7), (11, 0), (6, 1, 1), (16, 2, 4), (11, 4), (8, 1, 0, 6), (14, 1), (16, 2, 1),
    (11, 1), (16, 2, 2), (11, 2), (8, 1, 0, 7), (16, 2, 3), (11, 3), (12, 0), (16, 2, 6), (7, 2, 0), (16, 2, 5),
    (15, 2, 1), (14, 0), (11, 5), (13, 0), (16, 2, 7), (11, 6), (15, 2, 2), (8, 1, 2, 0), (11, 7), (6, 1, 2),
    (17, 1, 0), (15, 2, 3), (7, 2, 1), (7, 2, 2), (12, 1), (7, 2, 3), (15, 2, 4), (6, 1, 3), (13, 1), (17, 1, 1),
    (15, 2, 5), (15, 2, 6), (7, 2, 4), (7, 2, 5), (12, 2), (7, 2, 6), (13, 2), (17, 1, 2), (18, 0), (7, 2, 7),
    (8, 1, 2, 1), (15, 2, 7), (6, 1, 4), (8, 1, 2, 2), (18, 1), (12, 3), (13, 3), (17, 1, 3), (8, 1, 2, 3),
    (8, 1, 2, 4), (8, 1, 2, 5), (6, 1, 5), (8, 1, 2, 6), (8, 1, 2, 7), (14, 2), (17, 2, 0), (17, 2, 1), (17, 2, 2),
    (6, 1, 6), (17, 2, 3), (18, 2), (6, 1, 7), (12, 4), (13, 4), (17, 2, 4), (17, 1, 4), (18, 3), (12, 5), (13, 5),
    (17, 2, 5), (17, 1, 5), (12, 6), (13, 6), (17, 2, 6), (17, 1, 6), (18, 4), (12, 7), (13, 7), (17, 2, 7),
    (17, 1, 7), (18, 5), (18, 6), (18, 7),
)
OUTER = (
    (4, 0, 0), (0,), (4, 0, 1), (4, 0, 2), (4, 0, 3), (6, 0, 0), (10, 0), (6, 0, 1), (6, 0, 2), (4, 0, 4), (4, 0, 5),
    (4, 0, 6), (10, 1), (4, 0, 7), (6, 0, 3), (5, 0), (2, 0), (1,), (2, 1), (3, 0), (3, 1), (9, 0), (16, 0, 0),
    (11, 0), (16, 0, 1), (11, 1), (7, 0, 0), (10, 2), (7, 0, 1), (16, 0, 2), (6, 0, 4), (11, 2), (10, 3), (7, 0, 2),
    (16, 0, 3), (6, 0, 5), (10, 4), (7, 0, 3), (16, 0, 4), (6, 0, 6), (11, 3), (7, 0, 6), (11, 4), (10, 5), (7, 0, 4),
    (16, 0, 5), (7, 0, 5), (6, 0, 7), (11, 5), (10, 6), (16, 0, 6), (6, 1, 0), (11, 6), (10, 7), (4, 1, 0),
    (16, 0, 7), (6, 1, 1), (7, 0, 7), (4, 1, 1), (4, 1, 2), (6, 1, 2), (4, 1, 3), (12, 0), (4, 1, 4), (13, 0),
    (4, 1, 5), (6, 1, 3), (12, 1), (4, 1, 6), (6, 1, 4), (13, 1), (4, 1, 7), (12, 2), (6, 1, 5), (12, 3), (6, 1, 6),
    (13, 2), (12, 4), (6, 1, 7), (13, 3), (12, 5), (12, 6), (11, 7), (13, 4), (15, 0, 0), (8, 1, 0, 0), (12, 7),
    (13, 5), (15, 0, 1), (13, 6), (15, 0, 2), (8, 1, 0, 1), (15, 0, 3), (13, 7), (8, 1, 0, 3), (15, 0, 4), (15, 0, 5),
    (8, 1, 0, 2), (8, 1, 0, 4), (15, 0, 6), (8, 1, 0, 5), (8, 1, 0, 6), (15, 0, 7), (8, 1, 0, 7), (14, 0), (18, 0),
    (18, 1), (18, 2), (18, 3), (18, 4), (18, 5), (18, 6), (18, 7),
)
MESH = pl.DeviceIdType.MESH


def kernel(
    rows, cols, layers,
    left_ref, middle_ref, right_ref, out_ref,
    held, held2, rhs, sent, kept, near, far, near2,
    own_sem, home_sem, swap_sems, pair_sems, plane_sems, core_sems, near_sems, far_sems, near2_sems, hop_sems, relay_sems,
):
    group, side = rows // 2, cols // 2
    row, col, layer = lax.axis_index("row"), lax.axis_index("col"), lax.axis_index("layer")
    h, z = row // group, lax.rem(row, group)
    x, c = col // side, lax.rem(col, side)
    straight = h == x
    depth = middle_ref.shape[0]
    width = out_ref.shape[1]
    inner = left_ref.shape[1]
    chunk = left_ref.shape[0] // CHUNKS
    tile = min(TILE, width)

    def at(h_, x_):
        return (h_ * group + z, x_ * side + c, layer)

    def slot(col_, layer_):
        return col_ * layers + layer_

    sibling = col + 1 - 2 * lax.rem(col, 2)
    offsets = [(dc, dl) for dc in range(cols // 2) for dl in range(layers) if dc or dl]

    def moved(col_, dc, dl, sign):
        return lax.rem(col_ + sign * 2 * dc + cols, cols), lax.rem(layer + sign * dl + layers, layers)

    barrier = pltpu.get_barrier_semaphore()
    greeted = [at(1 - h, x), at(h, 1 - x), at(1 - h, 1 - x), (row, sibling, layer)]
    for shift in range(1, group):
        greeted.append((h * group + lax.rem(z + shift, group), col, layer))
    for dc, dl in offsets:
        greeted.append((row, *moved(col, dc, dl, 1)))
    for device in greeted:
        pl.semaphore_signal(barrier, inc=1, device_id=device, device_id_type=MESH)
    pl.semaphore_wait(barrier, len(greeted))

    me = slot(col, layer)

    def part(j):
        return pl.ds(j * chunk, chunk)

    def remote(src, dst, sems, device):
        return pltpu.make_async_remote_copy(
            src_ref=src, dst_ref=dst, send_sem=sems.at[0], recv_sem=sems.at[1],
            device_id=device, device_id_type=MESH,
        )

    home = pltpu.make_async_copy(left_ref, held.at[me], home_sem)

    def swap(j):
        device = at(1 - h, x) if j % 2 else at(h, 1 - x)
        return remote(left_ref.at[part(j)], near2.at[part(j)], swap_sems.at[j], device)

    def hop(j):
        device = at(h, 1 - x) if j % 2 else at(1 - h, x)
        target = slot((1 - x) * side + c, layer) if j % 2 else me
        return remote(near2.at[part(j)], held.at[target, part(j)], hop_sems.at[j], device)

    columns = pl.ds(pl.multiple_of(layer * width, width), width)
    pieces = CHUNKS
    step = depth // pieces

    def own(which):
        ref = (middle_ref, right_ref)[which]
        return pltpu.make_async_copy(
            ref.at[:, columns], rhs.at[which, pl.ds(z * depth, depth)], own_sem.at[which]
        )

    def pair(which, piece, shift):
        ref = (middle_ref, right_ref)[which]
        return remote(
            ref.at[pl.ds(piece * step, step), columns],
            rhs.at[which, pl.ds(z * depth + piece * step, step)],
            pair_sems.at[which, piece, shift - 1],
            (h * group + lax.rem(z + shift, group), col, layer),
        )

    def pair_start(which, piece):
        for shift in range(1, group):
            pair(which, piece, shift).start()

    def pair_wait(which):
        for piece in range(pieces):
            for shift in range(1, group):
                pair(which, piece, shift).wait_recv()
        own(which).wait()

    buffers = (held, held2)

    def spread(phase, j, index):
        dc, dl = offsets[index]
        ref = buffers[phase].at[me, part(j)]
        return remote(ref, ref, plane_sems.at[phase, j, index], (row, *moved(col, dc, dl, 1)))

    def pass_on(phase, j, index):
        origin = me
        if index:
            dc, dl = offsets[index - 1]
            origin = slot(*moved(col, dc, dl, -1))
        ref = buffers[phase].at[origin, part(j)]
        return remote(ref, ref, core_sems.at[phase, j, index], (row, sibling, layer))

    def spread_start(phase, j):
        for index in range(len(offsets)):
            spread(phase, j, index).start()
        pass_on(phase, j, 0).start()

    def spread_finish(phase, j):
        for index in range(len(offsets)):
            spread(phase, j, index).wait_recv()
            pass_on(phase, j, index + 1).start()
        for index in range(len(offsets) + 1):
            pass_on(phase, j, index).wait_recv()

    def multiply(phase, j, piece, target):
        blocks = side * layers
        ref = buffers[phase]

        @pl.loop(0, width // tile)
        def _(n):
            across = pl.ds(pl.multiple_of(n * tile, tile), tile)
            total = jnp.zeros((chunk, tile), jnp.float32)
            for k in range(blocks):
                total += jnp.dot(
                    ref[piece * blocks + k, part(j), :],
                    rhs[phase, pl.ds(k * inner, inner), across],
                    preferred_element_type=jnp.float32,
                )
            target[part(j), across] = total.astype(target.dtype)

    def add(one, two, j, store):
        @pl.loop(0, chunk // 32)
        def _(i):
            span = pl.ds(pl.multiple_of(j * chunk + i * 32, 32), 32)
            value = one[span, :].astype(jnp.float32) + two[span, :].astype(jnp.float32)
            store(span, value.astype(jnp.bfloat16))

    def near_copy(j):
        target_row = jnp.where(straight, h, x)
        target_col = jnp.where(straight, 1 - x, x)
        return remote(sent.at[part(j)], near.at[part(j)], near_sems.at[j], at(target_row, target_col))

    def far_copy(j):
        return remote(kept.at[part(j)], far.at[part(j)], far_sems.at[j], at(h, 1 - x))

    def relay_copy(j):
        return remote(far.at[part(j)], far.at[part(j)], relay_sems.at[j], at(1 - h, x))

    def near2_copy(j):
        return remote(sent.at[part(j)], near2.at[part(j)], near2_sems.at[j], at(1 - h, x))

    @pl.when(straight)
    def _():
        home.start()

    @pl.when(jnp.logical_not(straight))
    def _():
        for j in range(CHUNKS):
            swap(j).start()

    own(0).start()
    own(1).start()
    for piece in range(pieces):
        pair_start(0, piece)

    @pl.when(straight)
    def _():
        home.wait()

    for j in range(CHUNKS):
        @pl.when(straight)
        def _():
            swap(j).wait_recv()
            hop(j).start()

        @pl.when(jnp.logical_not(straight))
        def _():
            hop(j).wait_recv()

        spread_start(0, j)

    @pl.when(straight)
    def _():
        for j in range(CHUNKS):
            hop(j).wait_send()

    def first_done(j):
        near_copy(j).wait_recv()

        def store(span, value):
            held2[me, span, :] = value

        @pl.when(straight)
        def _():
            add(near, kept, j, store)

        @pl.when(jnp.logical_not(straight))
        def _():
            relay_copy(j).wait_recv()
            add(near, far, j, store)

        spread_start(1, j)

    for j in range(CHUNKS):
        spread_finish(0, j)
        if j == 0:
            pair_wait(0)
        multiply(0, j, h, kept)

        @pl.when(jnp.logical_not(straight))
        def _():
            far_copy(j).start()

        multiply(0, j, 1 - h, sent)
        near_copy(j).start()

        @pl.when(straight)
        def _():
            far_copy(j).wait_recv()
            relay_copy(j).start()

        pair_start(1, j)
        if j:
            first_done(j - 1)
    first_done(CHUNKS - 1)

    def out_done(j):
        near2_copy(j).wait_recv()

        def store(span, value):
            out_ref[span, :] = value

        add(near2, kept, j, store)

    for j in range(CHUNKS):
        spread_finish(1, j)
        if j == 0:
            pair_wait(1)
        near_copy(j).wait_send()

        @pl.when(jnp.logical_not(straight))
        def _():
            far_copy(j).wait_send()

        multiply(1, j, 1 - h, sent)
        near2_copy(j).start()
        multiply(1, j, h, kept)
        if j:
            out_done(j - 1)
    out_done(CHUNKS - 1)

    @pl.when(jnp.logical_not(straight))
    def _():
        for j in range(CHUNKS):
            swap(j).wait_send()

    @pl.when(straight)
    def _():
        for j in range(CHUNKS):
            relay_copy(j).wait_send()

    for j in range(CHUNKS):
        near2_copy(j).wait_send()
        for phase in range(2):
            for index in range(len(offsets)):
                spread(phase, j, index).wait_send()
            for index in range(len(offsets) + 1):
                pass_on(phase, j, index).wait_send()
    for which in range(2):
        for piece in range(pieces):
            for shift in range(1, group):
                pair(which, piece, shift).wait_send()


def wide_kernel(
    rows, cols, layers,
    left_ref, middle_ref, right_ref, out_ref, stage,
    a, b, part, cross, remote, pre, turned, far, fin,
    a_local, turn_sem, a_send, a_recv, pre_sems, own_sems, load_sems, bz_sems, by_sems,
    sx_sems, sc_sems, cross_sems, fwd_send, fwd_recv, o_send, o_recv, f_sems,
):
    group, side = rows // 2, cols // 2
    z, col, y = lax.axis_index("row"), lax.axis_index("col"), lax.axis_index("layer")
    x, c = col // side, lax.rem(col, side)
    h, par = z // group, lax.rem(z, group)
    straight = x == h
    crossed = jnp.logical_not(straight)
    inner = par != h
    mate = h * group + 1 - par
    near_z = (1 - h) * group + h
    far_z = (1 - h) * group + 1 - h
    depth = middle_ref.shape[0]
    width = middle_ref.shape[1]
    deep = left_ref.shape[1]
    half = left_ref.shape[0] // layers
    quarter = half // 2
    w = width // PIECES
    slabs = 3

    def at(z_, x_, c_, y_):
        return (z_, x_ * side + c_, y_)

    greeted = []
    for dx in range(2):
        for dc in range(2):
            for dy in range(2):
                if dx or dc or dy:
                    greeted.append(at(z, lax.rem(x + dx, 2), lax.rem(c + dc, 2), lax.rem(y + dy, 2)))
    for dz in range(1, rows):
        for dy in range(2):
            greeted.append(at(lax.rem(z + dz, rows), x, c, lax.rem(y + dy, 2)))
    barrier = pltpu.get_barrier_semaphore()
    for device in greeted:
        pl.semaphore_signal(barrier, inc=1, device_id=device, device_id_type=MESH)

    def send(src, dst, send_sem, recv_sem, device):
        return pltpu.make_async_remote_copy(
            src_ref=src, dst_ref=dst, send_sem=send_sem, recv_sem=recv_sem,
            device_id=device, device_id_type=MESH,
        )

    def when(flag, call, *args):
        @pl.when(flag)
        def _():
            call(*args)

    def left_rows(y_, s):
        return left_ref.at[pl.ds(pl.multiple_of(y_ * half + s * quarter, quarter), quarter)]

    def left_half(y_):
        return left_ref.at[pl.ds(pl.multiple_of(y_ * half, half), half)]

    def deep_cols(y_):
        return pl.ds(pl.multiple_of(y_ * deep, deep), deep)

    def rows_of(s):
        return pl.ds(pl.multiple_of(s * quarter, quarter), quarter)

    def a_piece(slab, s, y_):
        return a.at[0, slab, c, rows_of(s), deep_cols(y_)]

    def a_half(y_):
        return a.at[0, 0, c, :, deep_cols(y_)]

    there = jnp.where(inner, 1, 2)

    def keep_left():
        return pltpu.make_async_copy(left_half(y), a_half(y), a_local)

    def turn_kept():
        return send(left_half(1 - y), a_half(y), a_send.at[0], a_recv.at[0, y], at(z, x, c, 1 - y))

    def turn_sent():
        return send(left_half(1 - y), turned, a_send.at[0], turn_sem, at(z, x, c, 1 - y))

    def side_left(k):
        y_ = 1 - y if k else y
        return send(a_half(y_) if k else left_half(y), a_half(y_), a_send.at[1 + k], a_recv.at[0, y_], at(z, 1 - x, c, y))

    def give_left(k):
        src = turned.at[rows_of(1 - x)] if k else left_rows(y, 1 - x)
        return send(src, pre.at[k], a_send.at[1 + k], pre_sems.at[k], at(z, 1 - x, c, y))

    def jump(src, k):
        y_ = 1 - y if k else y
        return send(src, a_piece(there, x, y_), a_send.at[3 + k], a_recv.at[there, y_], at(near_z, x, c, y))

    def jump_left(k):
        return jump(turned.at[rows_of(x)] if k else left_rows(y, x), k)

    def left_start():
        @pl.when(straight)
        def _():
            turn_kept().start()
            side_left(0).start()
            keep_left().start()

        @pl.when(crossed)
        def _():
            turn_sent().start()
            give_left(0).start()

    def left_give():
        @pl.when(crossed)
        def _():
            turn_sent().wait_recv()
            give_left(1).start()

    def left_jump(k):
        @pl.when(crossed)
        def _():
            jump_left(k).start()

    def left_relay(k):
        @pl.when(straight)
        def _():
            give_left(k).wait_recv()
            jump(pre.at[k], k).start()

    def a_in(slab):
        def arrived(y_):
            ref = a_piece(slab, x, y_) if slab else a_half(y_)
            send(ref, ref, a_send.at[0], a_recv.at[slab, y_], at(z, x, c, 1 - y)).wait_recv()

        if slab:
            arrived(0)
            arrived(1)
            spread_x(0, slab, 0, x).start()
            spread_c(0, slab, 0, 0).start()
        else:
            @pl.when(straight)
            def _():
                arrived(1 - y)
                side_left(1).start()
                keep_left().wait()

            @pl.when(crossed)
            def _():
                arrived(0)
                arrived(1)

            whole(0).start()

    def a_block(phase, slab, s, n):
        if phase:
            return a.at[1, slab, c, rows_of(s), strip(n)]
        return a.at[0, slab, c, rows_of(s)]

    def spread_x(phase, slab, n, s):
        ref = a_block(phase, slab, s, n)
        k = n + phase
        return send(ref, ref, sx_sems.at[slab, k, 0], sx_sems.at[slab, k, 1], at(z, 1 - x, c, y))

    def spread_c(phase, slab, n, which):
        ref = a_block(phase, slab, 1 - x if which else x, n)
        k = n + phase
        return send(ref, ref, sc_sems.at[slab, k, which, 0], sc_sems.at[slab, k, which, 1], at(z, x, 1 - c, y))

    def whole(_):
        ref = a.at[0, 0, c]
        return send(ref, ref, sc_sems.at[0, 0, 0, 0], sc_sems.at[0, 0, 0, 1], at(z, x, 1 - c, y))

    def pass_on(phase, slab, n):
        spread_x(phase, slab, n, 1 - x).wait_recv()
        spread_c(phase, slab, n, 1).start()

    def a_ready(slab):
        if slab:
            for which in range(2):
                spread_c(0, slab, 0, which).wait_recv()
        else:
            whole(0).wait_recv()

    def a2_ready(slab):
        for n in range(PIECES):
            for which in range(2):
                spread_c(1, slab, n, which).wait_recv()

    sources = (middle_ref, right_ref)

    def strip(n):
        return pl.ds(n * w, w)

    def b_rows(plane, y_):
        return pl.ds(pl.multiple_of(plane * depth + y_ * (depth // 2), depth // 2), depth // 2)

    def b_slot(phase, n, plane, y_):
        if phase:
            return stage.at[n, b_rows(0, y_)]
        return b.at[n, b_rows(plane, y_)]

    def bz(phase, n):
        src = sources[phase].at[b_rows(0, y), strip(n)]
        return send(src, b_slot(phase, n, par, y), bz_sems.at[phase, n, 0], bz_sems.at[phase, n, 1], at(mate, x, c, y))

    def by(phase, n):
        ref = b_slot(phase, n, 1 - par, y)
        return send(ref, ref, by_sems.at[phase, n, 0], by_sems.at[phase, n, 1], at(z, x, c, 1 - y))

    def own(phase, n):
        rows_ = pl.ds(pl.multiple_of(par * depth, depth), depth)
        return pltpu.make_async_copy(sources[phase].at[:, strip(n)], b.at[n, rows_], own_sems.at[phase, n])

    def load(n):
        rows_ = pl.ds(pl.multiple_of((1 - par) * depth, depth), depth)
        return pltpu.make_async_copy(stage.at[n], b.at[n, rows_], load_sems.at[n])

    def b_send(phase, n):
        bz(phase, n).start()

    def b_turn(phase, n):
        bz(phase, n).wait_recv()
        by(phase, n).start()

    def b_ready(n):
        own(0, n).wait()
        by(0, n).wait_recv()

    def b_own(n):
        own(1, n).start()

    def b_load(n):
        by(0, n).wait_send()
        by(1, n).wait_recv()
        load(n).start()

    def b_loaded(n):
        own(1, n).wait()
        load(n).wait()

    def multiply(phase, slab, n, store):
        def add(k, total):
            deep_rows = pl.ds(pl.multiple_of(k * deep, deep), deep)
            cols_ = pl.ds(pl.multiple_of(lax.rem(k, 2) * deep, deep), deep)
            return total + jnp.dot(a[phase, slab, k // 2, :, cols_], b[n, deep_rows], preferred_element_type=jnp.float32)

        store(n, lax.fori_loop(0, 2 * depth // deep, add, jnp.zeros((half, w), jnp.float32)))

    def keep(slab):
        def store(n, total):
            part[slab, :, strip(n)] = total.astype(part.dtype)

        return store

    home_slab = (jnp.where(inner, 1, 2), 0, 0)
    home_z = (near_z, near_z, far_z)

    def cross_copy(slab, n):
        return send(
            part.at[slab, rows_of(1 - x), strip(n)], cross.at[slab, :, strip(n)],
            cross_sems.at[slab, n, 0], cross_sems.at[slab, n, 1], at(z, 1 - x, c, y),
        )

    def fwd_copy(slab, n, src):
        to = home_slab[slab]
        return send(
            src, remote.at[to, :, strip(n)], fwd_send.at[slab, n], fwd_recv.at[to, n],
            at(home_z[slab], x, c, y),
        )

    def fwd_part(slab, n):
        return fwd_copy(slab, n, part.at[slab, rows_of(x), strip(n)])

    def fwd_cross(slab, n):
        return fwd_copy(slab, n, cross.at[slab, :, strip(n)])

    def unit1(slab, n):
        multiply(0, slab, n, keep(slab))
        cross_copy(slab, n).start()

        @pl.when(crossed)
        def _():
            fwd_part(slab, n).start()

    def relay1(slab, n):
        @pl.when(straight)
        def _():
            cross_copy(slab, n).wait_recv()
            fwd_cross(slab, n).start()

    def reduce1(slab, n):
        ref = remote.at[slab, :, strip(n)]
        send(ref, ref, fwd_send.at[slab, n], fwd_recv.at[slab, n], at(z, x, c, 1 - y)).wait_recv()

        def add(other, base):
                @pl.loop(0, quarter // 32)
                def _(i):
                    span = pl.ds(pl.multiple_of(i * 32, 32), 32)
                    into = pl.ds(pl.multiple_of(x * quarter + i * 32, 32), 32)
                    mine = pl.ds(pl.multiple_of(base + i * 32, 32), 32)
                    value = other[slab, mine, strip(n)].astype(jnp.float32) + remote[slab, span, strip(n)].astype(jnp.float32)
                    a[1, slab, c, into, strip(n)] = value.astype(a.dtype)

        @pl.when(straight)
        def _():
            add(part, x * quarter)

        @pl.when(crossed)
        def _():
            cross_copy(slab, n).wait_recv()
            add(cross, 0)

        spread_x(1, slab, n, x).start()
        spread_c(1, slab, n, 0).start()

    def out_copy(slab, n):
        return send(
            part.at[slab, :, strip(n)], far.at[:, strip(n)], o_send.at[slab - 1, n], o_recv.at[n],
            at(home_z[slab], x, c, y),
        )

    def unit2(slab, n):
        cross_copy(slab, n).wait_send()
        fwd_part(slab, n).wait_send()
        multiply(1, slab, n, keep(slab))
        out_copy(slab, n).start()

    my_rows = pl.ds(pl.multiple_of(y * half, half), half)

    def fin_copy(n):
        cols_ = pl.ds(n % (PIECES // 2) * w, w)
        return send(fin.at[n], out_ref.at[my_rows, cols_], f_sems.at[n, 0], f_sems.at[n, 1], at(z, x, c, 1 - y))

    def unit3(n):
        ref = far.at[:, strip(n)]
        send(ref, ref, o_send.at[0, n], o_recv.at[n], at(z, x, c, 1 - y)).wait_recv()

        def store(n, total):
            value = total + far[:, strip(n)].astype(jnp.float32)
            fin[n] = value.astype(fin.dtype)

        multiply(1, 0, n, store)
        mine = y == n // (PIECES // 2)

        @pl.when(mine)
        def _():
            out_ref[my_rows, pl.ds(n % (PIECES // 2) * w, w)] = fin[n]

        @pl.when(jnp.logical_not(mine))
        def _():
            fin_copy(n).start()

    steps = (
        left_start, left_give, left_jump, left_relay, b_send, a_in, b_turn, relay1, pass_on, a_ready,
        b_ready, b_own, b_load, b_loaded, a2_ready, reduce1, unit1, unit2, unit3,
    )
    for n in range(PIECES):
        own(0, n).start()
    pl.semaphore_wait(barrier, len(greeted))

    def follow(order):
        for step, *args in order:
            steps[step](*args)

    when(inner, follow, INNER)
    when(jnp.logical_not(inner), follow, OUTER)

    for n in range(PIECES):
        mine = y == n // (PIECES // 2)

        @pl.when(mine)
        def _():
            fin_copy(n).wait_recv()

        @pl.when(jnp.logical_not(mine))
        def _():
            fin_copy(n).wait_send()

    @pl.when(straight)
    def _():
        turn_kept().wait_send()
        for k in range(2):
            side_left(k).wait_send()
            jump(pre.at[k], k).wait_send()

    @pl.when(crossed)
    def _():
        turn_sent().wait_send()
        for k in range(2):
            give_left(k).wait_send()
            jump_left(k).wait_send()

    for phase in range(2):
        for n in range(PIECES):
            bz(phase, n).wait_send()
            if phase:
                by(phase, n).wait_send()

    def sent(slab):
        if slab:
            spread_x(0, slab, 0, x).wait_send()
            for which in range(2):
                spread_c(0, slab, 0, which).wait_send()
        else:
            whole(0).wait_send()
        for n in range(PIECES):
            spread_x(1, slab, n, x).wait_send()
            for which in range(2):
                spread_c(1, slab, n, which).wait_send()
            if slab:
                out_copy(slab, n).wait_send()
            else:
                cross_copy(slab, n).wait_send()
                fwd_part(slab, n).wait_send()

    sent(0)
    for slab in range(1, slabs):
        when(inner, sent, slab)


def wide(rows, cols, layers, left, middle, right):
    height, inner = left.shape
    depth, width = middle.shape
    half = height // layers
    quarter = half // 2
    bf16 = jnp.bfloat16
    anywhere = pl.BlockSpec(memory_space=pl.ANY)
    dma = pltpu.SemaphoreType.DMA
    out, _ = pl.pallas_call(
        functools.partial(wide_kernel, rows, cols, layers),
        out_shape=(
            jax.ShapeDtypeStruct((height, width // layers), bf16),
            jax.ShapeDtypeStruct((PIECES, depth, width // PIECES), bf16),
        ),
        in_specs=[anywhere] * 3,
        out_specs=(pl.BlockSpec(memory_space=pltpu.VMEM), anywhere),
        scratch_shapes=[
            pltpu.VMEM((2, 3, 2, half, depth), bf16),
            pltpu.VMEM((PIECES, 2 * depth, width // PIECES), bf16),
            pltpu.VMEM((3, half, width), bf16),
            pltpu.VMEM((3, quarter, width), bf16),
            pltpu.VMEM((3, quarter, width), bf16),
            pltpu.VMEM((2, quarter, inner), bf16),
            pltpu.VMEM((half, inner), bf16),
            pltpu.VMEM((half, width), bf16),
            pltpu.VMEM((PIECES, half, width // PIECES), bf16),
            dma,
            dma,
            dma((5,)),
            dma((3, 2)),
            dma((2,)),
            dma((2, PIECES)),
            dma((PIECES,)),
            dma((2, PIECES, 2)),
            dma((2, PIECES, 2)),
            dma((3, PIECES + 1, 2)),
            dma((3, PIECES + 1, 2, 2)),
            dma((3, PIECES, 2)),
            dma((3, PIECES)),
            dma((3, PIECES)),
            dma((2, PIECES)),
            dma((PIECES,)),
            dma((PIECES, 2)),
        ],
        compiler_params=pltpu.CompilerParams(
            collective_id=0, has_side_effects=True, vmem_limit_bytes=67043328
        ),
    )(left, middle, right)
    return out


def per_device(left, middle, right):
    rows, cols, layers = (lax.axis_size(name) for name in ("row", "col", "layer"))
    height, inner = left.shape
    width = right.shape[1] // layers
    depth = right.shape[0]
    group = rows // 2
    if (rows, cols, layers) == (2 * PAIR, 2 * PAIR, PAIR) and depth == layers * inner:
        return wide(rows, cols, layers, left, middle, right)
    partners = cols // 2 * layers - 1
    bf16 = jnp.bfloat16
    anywhere = pl.BlockSpec(memory_space=pl.ANY)
    dma = pltpu.SemaphoreType.DMA
    return pl.pallas_call(
        functools.partial(kernel, rows, cols, layers),
        out_shape=jax.ShapeDtypeStruct((height, width), bf16),
        in_specs=[anywhere] * 3,
        out_specs=pl.BlockSpec(memory_space=pltpu.VMEM),
        scratch_shapes=[
            pltpu.VMEM((cols * layers, height, inner), bf16),
            pltpu.VMEM((cols * layers, height, inner), bf16),
            pltpu.VMEM((2, group * depth, width), bf16),
        ]
        + [pltpu.VMEM((height, width), bf16)] * 5
        + [
            dma((2,)),
            dma,
            dma((CHUNKS, 2)),
            dma((2, CHUNKS, max(group - 1, 1), 2)),
            dma((2, CHUNKS, partners, 2)),
            dma((2, CHUNKS, partners + 1, 2)),
            dma((CHUNKS, 2)),
            dma((CHUNKS, 2)),
            dma((CHUNKS, 2)),
            dma((CHUNKS, 2)),
            dma((CHUNKS, 2)),
        ],
        compiler_params=pltpu.CompilerParams(
            collective_id=0, has_side_effects=True, vmem_limit_bytes=67043328
        ),
    )(left, middle, right)


def solution(mesh):
    return jax.shard_map(
        per_device,
        mesh=mesh,
        in_specs=(P("row", ("col", "layer")), P("row", "col"), P("row", "col")),
        out_specs=P("row", ("col", "layer")),
        check_vma=False,
    )
```
